32 devices in a mesh: grp: 4 (over z), ctx: 2 (over y), wid: 4 (over x, core).
Axes of the slice: x: 2, y: 2, z: 4, core: 2. Of those that a mesh axis runs over, the one named last changes fastest.
Arguments:
- query: bfloat16 [256, 64, 128], P(None, 'wid'), may hold values from -64 to 64
- keys: bfloat16 [4, 512, 8, 128], P(None, ('grp', 'ctx'), 'wid'), may hold values from -64 to 64
- values: bfloat16 [4, 512, 8, 128], P(None, ('grp', 'ctx'), 'wid'), may hold values from -6 to 6
- lengths: int32 [4, 8], replicated, may hold values from 32 to 64
- query_pos: int32 [256], replicated, may hold values from 128 to 511
- resid: bfloat16 [256, 5120], P('wid', ('grp', 'ctx')), may hold values from -1.1953125 to 1.1953125
- out_weight: bfloat16 [8192, 5120], P('wid', ('grp', 'ctx')), may hold values from -0.0625 to 0.0625
- enc_weight: bfloat16 [5120, 24576], P('wid', ('grp', 'ctx')), may hold values from -0.078125 to 0.078125
- enc_bias: float32 [24576], P(('grp', 'ctx')), may hold values from -3 to 3
- dec_weight: bfloat16 [24576, 5120], P(('grp', 'ctx'), 'wid'), may hold values from -0.078125 to 0.078125
- dec_bias: float32 [5120], P('wid'), may hold values from -3 to 3
Outputs:
- layer_out: bfloat16 [256, 5120], P('wid', ('grp', 'ctx'))
- enc_grad: bfloat16 [5120, 24576], P('wid', ('grp', 'ctx'))
- enc_bias_grad: float32 [24576], P(('grp', 'ctx'))
- dec_grad: bfloat16 [24576, 5120], P(('grp', 'ctx'), 'wid')
- dec_bias_grad: float32 [5120], P('wid')
The draws below stay inside these ranges and needn't reach their ends.
Inputs may be any that keep to these rules, and one draw needn't show every extreme that they name: `lengths`: live slots of a shard are its first ones.
All inputs are finite; a program needn't handle non-finite values.
Results may differ from the reference program's by a relative error of at most 0.024.
Values may be sent and summed in bfloat16 or wider, within the bound.
A program may use at most 128 MiB of HBM per device.

```python
import jax
import jax.numpy as jnp
from jax import lax

D = 5120
QH = 64
KVH = 8
HD = 128
LAT = 24576
SEQS = 4
ROWS_SEQ = 64
SLOTS = 64
GQA = 8
SHARDS = 8
CACHE = 512
ROWS = 256


def query_and_keys(key):
    base = jax.random.fold_in(key, 11)
    key_query, key_keys = jax.random.split(base, 2)
    query = 2.0 * jax.random.normal(key_query, (ROWS, QH, HD), jnp.float32)
    cached = jax.random.normal(key_keys, (SEQS, CACHE, KVH, HD), jnp.float32)
    return (query, cached)


def draw_query(key, part):
    return query_and_keys(key)[0].astype(jnp.bfloat16)


def draw_keys(key, part):
    return query_and_keys(key)[1].astype(jnp.bfloat16)


def plant(result, rng, low, high):
    spot = [jax.random.randint(jax.random.fold_in(rng, axis), (), 0, length) for axis, length in enumerate(result.shape)]
    main_axis = result.shape.index(max(result.shape))
    neighbour = spot[:main_axis] + [(spot[main_axis] + 1) % result.shape[main_axis]] + spot[main_axis + 1:]
    return result.at[tuple(spot)].set(low).at[tuple(neighbour)].set(high)


def block_levels(stream_key, extent, pieces, least, largest):
    loudness, own = 1.0, jax.random.fold_in(stream_key, 6)
    for dim, blocks in pieces:
        steps = jnp.exp(jax.random.uniform(jax.random.fold_in(own, dim), (blocks,), jnp.float32, least / len(pieces), largest / len(pieces)))
        loudness = loudness * jnp.repeat(steps, extent[dim] // blocks).reshape([-1 if axis == dim else 1 for axis in range(len(extent))])
    return loudness


def normal_values(rng, shape, spread, bound, cuts=(), kind=jnp.bfloat16):
    loudness = block_levels(rng, shape, cuts, -0.22, 0.18) if cuts else 1.0
    drawn = jax.random.normal(rng, shape, jnp.float32) * spread * loudness
    return jnp.minimum(jnp.maximum(drawn, -bound), bound).astype(kind)


def setup_inputs(seed: int = 0) -> dict:
    arg_keys = jax.random.split(jax.random.key(seed), 12)
    return {
        "query": draw_query(jax.random.fold_in(arg_keys[11], 71), 0),
        "keys": draw_keys(jax.random.fold_in(arg_keys[11], 71), 0),
        "values": normal_values(arg_keys[2], (SEQS, CACHE, KVH, HD), 1.0, 6.0, ((1, 8), (2, 4))),
        "lengths": plant(jax.random.randint(arg_keys[3], (SEQS, SHARDS), SLOTS // 2, SLOTS + 1), jax.random.fold_in(arg_keys[3], 1), SLOTS // 2, SLOTS).astype(jnp.int32),
        "query_pos": plant(jax.random.randint(arg_keys[4], (ROWS,), SHARDS * SLOTS // 4, SHARDS * SLOTS), jax.random.fold_in(arg_keys[4], 1), SHARDS * SLOTS // 4, (SHARDS * SLOTS) - 1).astype(jnp.int32),
        "resid": normal_values(arg_keys[5], (ROWS, D), 0.2, 1.1953125, ((0, 4), (1, 8))),
        "out_weight": normal_values(arg_keys[6], (QH * HD, D), (QH * HD) ** -0.5, 0.0625, ((0, 4), (1, 8))),
        "enc_weight": normal_values(arg_keys[7], (D, LAT), D ** -0.5, 0.078125, ((0, 4), (1, 8))),
        "enc_bias": normal_values(arg_keys[8], (LAT,), 0.5, 3.0, ((0, 8),), jnp.float32),
        "dec_weight": normal_values(arg_keys[9], (LAT, D), D ** -0.5, 0.078125, ((0, 8), (1, 4))),
        "dec_bias": normal_values(arg_keys[10], (D,), 0.5, 3.0, ((0, 4),), jnp.float32),
    }


def one_sequence(items):
    q_seq, k_seq, v_seq, key_pos, live_slot, row_position = items
    scores = jnp.einsum("rkgd,tkd->krgt", q_seq.astype(jnp.float32), k_seq.astype(jnp.float32),
                        precision=lax.Precision.HIGHEST) * (HD ** -0.5)
    visible = live_slot[None, :] & (key_pos[None, :] <= row_position[:, None])
    visible_mask = visible[None, :, None, :]
    peak = jnp.max(jnp.where(visible_mask, scores, -1e30), axis=-1)
    weights = jnp.where(visible_mask, jnp.exp(scores - peak[..., None]), 0.0)
    weight_sum = jnp.sum(weights, axis=-1)
    weights_low = lax.optimization_barrier(weights.astype(jnp.bfloat16)).astype(jnp.float32)
    weighted = jnp.einsum("krgt,tkd->rkgd", weights_low, v_seq.astype(jnp.float32),
                          precision=lax.Precision.HIGHEST)
    return weighted / jnp.transpose(weight_sum, (1, 0, 2))[..., None]


def reference(query, keys, values, lengths, query_pos, resid, out_weight, enc_weight, enc_bias, dec_weight, dec_bias):
    slot_ids = jnp.arange(SLOTS, dtype=jnp.int32)
    offsets = (jnp.cumsum(lengths, axis=1) - lengths).astype(jnp.int32)
    key_pos = (offsets[:, :, None] + slot_ids[None, None, :]).astype(jnp.int32).reshape(SEQS, CACHE)
    live_slot = (slot_ids[None, None, :] < lengths[:, :, None]).reshape(SEQS, CACHE)
    q_view = query.reshape(SEQS, ROWS_SEQ, KVH, GQA, HD)
    row_position = query_pos.reshape(SEQS, ROWS_SEQ)
    attn = lax.map(one_sequence, (q_view, keys, values, key_pos, live_slot, row_position))
    attention = attn.astype(jnp.bfloat16).reshape(ROWS, QH * HD)
    layer_out = (jnp.dot(attention, out_weight, preferred_element_type=jnp.float32)
                 + resid.astype(jnp.float32)).astype(jnp.bfloat16)
    preact = jnp.dot(layer_out, enc_weight, preferred_element_type=jnp.float32) + enc_bias
    latents = (jax.nn.softplus(4.0 * preact) * 0.25).astype(jnp.bfloat16)
    recon = jnp.dot(latents, dec_weight, preferred_element_type=jnp.float32)
    scaled_error = ((recon + dec_bias - layer_out.astype(jnp.float32)) * (ROWS ** -0.5)).astype(jnp.bfloat16)
    dec_grad = lax.dot_general(latents, scaled_error, (((0,), (0,)), ((), ())),
                               preferred_element_type=jnp.float32).astype(jnp.bfloat16)
    dec_bias_grad = jnp.sum(scaled_error.astype(jnp.float32), axis=0)
    latent_grad = lax.dot_general(scaled_error, dec_weight, (((1,), (1,)), ((), ())),
                                  preferred_element_type=jnp.float32)
    preact_grad = (latent_grad * jax.nn.sigmoid(4.0 * preact)).astype(jnp.bfloat16)
    enc_grad = lax.dot_general(layer_out, preact_grad, (((0,), (0,)), ((), ())),
                               preferred_element_type=jnp.float32).astype(jnp.bfloat16)
    enc_bias_grad = jnp.sum(preact_grad.astype(jnp.float32), axis=0)
    return layer_out, enc_grad, enc_bias_grad, dec_grad, dec_bias_grad
```

```python
import functools

import jax
import jax.numpy as jnp
from jax import lax
from jax.experimental import pallas as pl
from jax.experimental.pallas import tpu as pltpu
from jax.sharding import PartitionSpec as P

HD = 128
MESH = pl.DeviceIdType.MESH


def exchange_kernel(n, where, peer_id, gather, x_ref, out_ref, send_sem, recv_sem):
    me = where()
    peers = [lax.rem(me + step, n) for step in range(1, n)]
    barrier = pltpu.get_barrier_semaphore()
    for peer in peers:
        pl.semaphore_signal(barrier, inc=1, device_id=peer_id(peer), device_id_type=MESH)
    pl.semaphore_wait(barrier, n - 1)

    def copy_to(step, peer):
        return pltpu.make_async_remote_copy(
            src_ref=x_ref if gather else x_ref.at[peer],
            dst_ref=out_ref.at[me],
            send_sem=send_sem.at[step],
            recv_sem=recv_sem.at[me],
            device_id=peer_id(peer),
            device_id_type=MESH,
        )

    def copy_from(step, peer):
        return pltpu.make_async_remote_copy(
            src_ref=x_ref if gather else x_ref.at[peer],
            dst_ref=out_ref.at[peer],
            send_sem=send_sem.at[step],
            recv_sem=recv_sem.at[peer],
            device_id=peer_id(peer),
            device_id_type=MESH,
        )

    sends = [copy_to(step, peer) for step, peer in enumerate(peers)]
    for copy in sends:
        copy.start()
    out_ref[me] = x_ref[...] if gather else x_ref[me]
    for step, peer in enumerate(peers):
        copy_from(step, peer).wait_recv()
    for copy in sends:
        copy.wait_send()


def exchange(x, n, where, peer_id, gather, number):
    block = x.shape if gather else x.shape[1:]
    return pl.pallas_call(
        functools.partial(exchange_kernel, n, where, peer_id, gather),
        out_shape=jax.ShapeDtypeStruct((n,) + block, x.dtype),
        in_specs=[pl.BlockSpec(memory_space=pltpu.VMEM)],
        out_specs=pl.BlockSpec(memory_space=pltpu.VMEM),
        scratch_shapes=[pltpu.SemaphoreType.DMA((n,)), pltpu.SemaphoreType.DMA((n,))],
        compiler_params=pltpu.CompilerParams(
            collective_id=number, has_side_effects=True, vmem_limit_bytes=24 * 1024 * 1024
        ),
        name="exchange%d" % number,
    )(x)


class Groups:
    def __init__(self, sizes):
        ctx_n = sizes["ctx"]
        self.shards = (
            sizes["grp"] * ctx_n,
            lambda: lax.axis_index("grp") * ctx_n + lax.axis_index("ctx"),
            lambda p: {"grp": p // ctx_n, "ctx": lax.rem(p, ctx_n)},
        )
        self.wid = (sizes["wid"], lambda: lax.axis_index("wid"), lambda p: {"wid": p})
        self.low = (
            2,
            lambda: lax.rem(lax.axis_index("wid"), 2),
            lambda p: {"wid": (lax.axis_index("wid") // 2) * 2 + p},
        )
        self.high = (
            sizes["wid"] // 2,
            lambda: lax.axis_index("wid") // 2,
            lambda p: {"wid": p * 2 + lax.rem(lax.axis_index("wid"), 2)},
        )


def scatter_sum(x, group, number):
    n = group[0]
    parts = exchange(x.reshape((n, x.shape[0] // n) + x.shape[1:]), *group, False, number)
    return jnp.sum(parts.astype(jnp.float32), axis=0)


def gather_rows(x, group, number):
    whole = exchange(x, *group, True, number)
    return whole.reshape((whole.shape[0] * whole.shape[1],) + whole.shape[2:])


def attend(groups, query, keys, values, lengths, query_pos):
    seq_count, slot_count, kv_local, head_dim = keys.shape
    row_count, heads_local = query.shape[:2]
    group_size = heads_local // kv_local
    shards = groups.shards[0]
    pairs = seq_count * kv_local
    chunks = shards // pairs
    rows = row_count // seq_count // chunks
    pair = lax.axis_index(("grp", "ctx")) // chunks
    seq, head = pair // kv_local, lax.rem(pair, kv_local)
    row0 = seq * (row_count // seq_count) + lax.rem(lax.axis_index(("grp", "ctx")), chunks) * rows
    cache = jnp.concatenate([keys, values], axis=-1).transpose(0, 2, 1, 3)
    cache = cache.reshape(pairs, slot_count, 2 * head_dim)
    if chunks > 1:
        cache = jnp.repeat(cache, chunks, axis=0)
    cache = exchange(cache, *groups.shards, False, 0).reshape(shards * slot_count, 2 * head_dim)
    q = lax.dynamic_slice(query, (row0, head * group_size, 0), (rows, group_size, head_dim))
    live = lax.dynamic_index_in_dim(lengths, seq, 0, keepdims=False)
    before = jnp.arange(shards)[None, :] < jnp.arange(shards)[:, None]
    offset = jnp.sum(jnp.where(before, live[None, :], 0), axis=1)
    slot_ids = jnp.arange(slot_count, dtype=jnp.int32)
    key_pos = jnp.where(
        slot_ids[None, :] < live[:, None], offset[:, None] + slot_ids[None, :], jnp.int32(2**30)
    ).reshape(-1)
    position = lax.dynamic_slice_in_dim(query_pos, row0, rows, 0)
    visible = (key_pos[None, :] <= position[:, None])[:, None, :]
    scores = jnp.einsum(
        "rgd,td->rgt", q, cache[:, :head_dim], preferred_element_type=jnp.float32
    ) * HD ** (-0.5)
    peak = jnp.max(jnp.where(visible, scores, -1e30), axis=-1, keepdims=True)
    weights = jnp.where(visible, jnp.exp(scores - peak), 0.0)
    weight_sum = jnp.sum(weights, axis=-1, keepdims=True)
    weighted = jnp.einsum(
        "rgt,td->rgd", weights.astype(jnp.bfloat16), cache[:, head_dim:],
        preferred_element_type=jnp.float32,
    )
    mine = (weighted / weight_sum).astype(jnp.bfloat16).reshape(rows, group_size * head_dim)
    attention = exchange(mine, *groups.shards, True, 1)
    attention = attention.reshape(seq_count, kv_local, chunks, rows, group_size * head_dim)
    return attention.transpose(0, 2, 3, 1, 4).reshape(row_count, heads_local * head_dim)


def body(
    sizes,
    query,
    keys,
    values,
    lengths,
    query_pos,
    resid,
    out_weight,
    enc_weight,
    enc_bias,
    dec_weight,
    dec_bias,
):
    groups = Groups(sizes)
    row_count = query.shape[0]
    shard_pos = lax.axis_index(("grp", "ctx"))
    attention = attend(groups, query, keys, values, lengths, query_pos)
    projected = jnp.dot(attention, out_weight, preferred_element_type=jnp.float32)
    mixed = scatter_sum(projected.astype(jnp.bfloat16), groups.wid, 2)
    layer_out = (mixed + resid.astype(jnp.float32)).astype(jnp.bfloat16)
    rows, cols = layer_out.shape
    wid_n = sizes["wid"]
    wide = exchange(layer_out, *groups.shards, True, 3)
    wide = wide.reshape(wid_n, -1, rows, cols).transpose(0, 2, 1, 3).reshape(wid_n, rows, -1)
    block = exchange(wide, *groups.wid, False, 4).reshape(row_count, -1)
    enc_part = jnp.dot(block, enc_weight, preferred_element_type=jnp.float32)
    preact = scatter_sum(enc_part.astype(jnp.bfloat16), groups.low, 5).astype(jnp.bfloat16)
    preact = scatter_sum(preact, groups.high, 6) + enc_bias
    my_latents = (jax.nn.softplus(4.0 * preact) * 0.25).astype(jnp.bfloat16)
    latents = gather_rows(gather_rows(my_latents, groups.high, 7), groups.low, 8)
    row_scale = row_count ** (-0.5)
    recon = jnp.dot(latents, dec_weight, preferred_element_type=jnp.float32)
    recon = scatter_sum(recon.astype(jnp.bfloat16), groups.shards, 9)
    piece_len = recon.shape[0]
    target = lax.dynamic_slice_in_dim(block, shard_pos * piece_len, piece_len, 0).astype(
        jnp.float32
    )
    scaled_error = ((recon + dec_bias - target) * row_scale).astype(jnp.bfloat16)
    error_all = gather_rows(scaled_error, groups.shards, 10)
    dec_bias_grad = jnp.sum(error_all, axis=0, dtype=jnp.float32)
    latent_part = lax.dot_general(
        error_all, dec_weight, (((1,), (1,)), ((), ())), preferred_element_type=jnp.float32
    )
    dec_grad = lax.dot_general(
        latents, error_all, (((0,), (0,)), ((), ())), preferred_element_type=jnp.float32
    )
    latent_grad = scatter_sum(latent_part.astype(jnp.bfloat16), groups.low, 11).astype(jnp.bfloat16)
    latent_grad = scatter_sum(latent_grad, groups.high, 12)
    my_grad = (latent_grad * jax.nn.sigmoid(4.0 * preact)).astype(jnp.bfloat16)
    preact_grad = gather_rows(gather_rows(my_grad, groups.high, 13), groups.low, 14)
    enc_grad = lax.dot_general(
        block, preact_grad, (((0,), (0,)), ((), ())), preferred_element_type=jnp.float32
    ).astype(jnp.bfloat16)
    enc_bias_grad = jnp.sum(preact_grad, axis=0, dtype=jnp.float32)
    return (layer_out, enc_grad, enc_bias_grad, dec_grad.astype(jnp.bfloat16), dec_bias_grad)


def solution(mesh):
    placed = (
        P(None, "wid", None),
        P(None, ("grp", "ctx"), "wid", None),
        P(None, ("grp", "ctx"), "wid", None),
        P(),
        P(),
        P("wid", ("grp", "ctx")),
        P("wid", ("grp", "ctx")),
        P("wid", ("grp", "ctx")),
        P(("grp", "ctx")),
        P(("grp", "ctx"), "wid"),
        P("wid"),
    )
    return jax.shard_map(
        functools.partial(body, dict(mesh.shape)),
        mesh=mesh,
        in_specs=placed,
        out_specs=(
            P("wid", ("grp", "ctx")),
            P("wid", ("grp", "ctx")),
            P(("grp", "ctx")),
            P(("grp", "ctx"), "wid"),
            P("wid"),
        ),
        check_vma=False,
    )
```
